16 devices in a mesh: rep: 1, dp: 16 (over x, y, z, core).
Axes of the slice: x: 2, y: 2, z: 2, core: 2. Of those that a mesh axis runs over, the one named last changes fastest.
Arguments:
- a: bfloat16 [16, 4, 4096, 1024], P(('rep', 'dp'))
- g: bfloat16 [16, 4, 4096, 3200], P(('rep', 'dp'))
Outputs:
- output: bfloat16 [4, 1024, 3200], P('rep')
All inputs are finite; a program needn't handle non-finite values.
Results may differ from the reference program's by a relative error of at most 0.012.
Values are sent between devices in bfloat16 or wider.
A program may use at most 2 GiB of HBM per device.

```python
import jax
import jax.numpy as jnp
from jax import lax

DEVICES = 16
MATRICES = 4
TOKENS = 4096
D = 1024
FF = 3200


def setup_inputs(seed: int = 0, part: int = 0) -> dict:
    ka, kg, ks = (jax.random.fold_in(k, part) for k in jax.random.split(jax.random.key(seed), 3))
    size = 2.0 ** jax.random.uniform(ks, (DEVICES, MATRICES, 1, 1), jnp.float32, -1.0, 1.0)
    a = jax.random.normal(ka, (DEVICES, MATRICES, TOKENS, D), jnp.float32)
    g = size * jax.random.normal(kg, (DEVICES, MATRICES, TOKENS, FF), jnp.float32) * (DEVICES * TOKENS) ** -0.5
    return {"a": a.astype(jnp.bfloat16), "g": g.astype(jnp.bfloat16)}


def reference(a, g):
    def take(so_far, one):
        return so_far + jnp.einsum("ntd,ntf->ndf", *one, preferred_element_type=jnp.float32), None

    return lax.scan(take, jnp.zeros((MATRICES, D, FF), jnp.float32), (a, g))[0].astype(jnp.bfloat16)
```

```python
import functools

import jax
import jax.numpy as jnp
from jax import lax
from jax.experimental import pallas as pl
from jax.experimental.pallas import tpu as pltpu
from jax.sharding import PartitionSpec as P

MESH = pl.DeviceIdType.MESH
F32 = jnp.float32
BF16 = jnp.bfloat16

N, T, D, F = 4, 4096, 1024, 3200
H = D // 2
W = 512
PER = F // W
REM = F - PER * W
CH = N * PER
NCH = CH + 1
PARTS = 4
PR = H // PARTS
TB = 512
R = 4
RA = 6
D1, D2, D3, D4, D5, D6, D7, D8 = 1, 3, 4, 5, 6, 8, 10, 12


def main_kernel(a_ref, g_ref, out_ref, aT, ast, gv, grem, acc, xacc, sb0, rb0, sb1, rb1, sb2, rb2, sb3, rb3, fb,
                ssem, rsem, asem, gsem, remsem, lsem):
    me = lax.axis_index("dp")
    core = me % 2
    other = me + 1 - 2 * core

    def stride(d):
        return 8 - 5 * d + d * d

    def bit(d):
        return (me // stride(d)) % 2

    def partner(d):
        return me + stride(d) * (1 - 2 * bit(d))

    barrier = pltpu.get_barrier_semaphore()
    for peer in (other, partner(0), partner(1), partner(2)):
        pl.semaphore_signal(barrier, inc=1, device_id={"dp": peer}, device_id_type=MESH)

    def dim(p, k, i):
        rot = p if p < 3 else k % 3
        return (rot + i) % 3

    def rows(x, m):
        return pl.multiple_of(x, m)

    def remote(src, dst, ph, r, p, peer):
        return pltpu.make_async_remote_copy(
            src_ref=src, dst_ref=dst, send_sem=ssem.at[ph, r, p], recv_sem=rsem.at[ph, r, p],
            device_id={"dp": peer}, device_id_type=MESH)

    def a_copy(n, q, slot):
        return pltpu.make_async_copy(a_ref.at[0, n, pl.ds(rows(q * TB, TB), TB), :], ast.at[slot], asem.at[slot])

    def g_copy(k):
        n, j = k // PER, k % PER
        return pltpu.make_async_copy(g_ref.at[0, n, :, pl.ds(pl.multiple_of(j * W, W), W)], gv.at[k % 2], gsem.at[k % 2])

    def rem_copy(n):
        return pltpu.make_async_copy(g_ref.at[0, n, :, pl.ds(PER * W, REM)], grem, remsem)

    def transpose(n, q, slot):
        aT[n % 2, :, pl.ds(rows(q * TB, TB), TB)] = ast[slot].T

    for q in range(2):
        a_copy(0, q, q).start()
    g_copy(0).start()

    def first(q, _):
        a_copy(0, q, q % 2).wait()
        transpose(0, q, q % 2)

        @pl.when(q + 2 < T // TB)
        def _():
            a_copy(0, q + 2, q % 2).start()
        return 0

    lax.fori_loop(0, T // TB, first, 0)
    pl.semaphore_wait(barrier, 4)

    def x0(k):
        r = k % R
        return remote(sb0.at[r], rb0.at[r], 0, r, 0, other)

    def x1(k, p):
        r = k % R
        return remote(sb1.at[r, p], rb1.at[r, p], 1, r, p, partner(dim(p, k, 0)))

    def x2(k, p):
        r = k % R
        return remote(sb2.at[r, p], rb2.at[r, p], 2, r, p, partner(dim(p, k, 1)))

    def x3(k, p):
        r = k % R
        return remote(sb3.at[r, p], rb3.at[r, p], 3, r, p, partner(dim(p, k, 2)))

    def offs(k, p):
        o1 = p * PR + bit(dim(p, k, 0)) * (PR // 2)
        o2 = o1 + bit(dim(p, k, 1)) * (PR // 4)
        o3 = o2 + bit(dim(p, k, 2)) * (PR // 8)
        return o1, o2, o3

    def block(k, o, m):
        return out_ref.at[k, pl.ds(rows(core * H + o, m), m), :]

    def own(k, p):
        return pltpu.make_async_copy(fb.at[k % R, p], block(k, offs(k, p)[2], PR // 8), lsem.at[k % R, p])

    def y1(k, p):
        return remote(fb.at[k % R, p], block(k, offs(k, p)[2], PR // 8), 4, k % R, p, partner(dim(p, k, 2)))

    def y2(k, p):
        b = block(k, offs(k, p)[1], PR // 4)
        return remote(b, b, 5, k % R, p, partner(dim(p, k, 1)))

    def y3(k, p):
        b = block(k, offs(k, p)[0], PR // 2)
        return remote(b, b, 6, k % R, p, partner(dim(p, k, 0)))

    def y4(k):
        b = block(k, 0, H)
        return remote(b, b, 7, k % R, 0, other)

    def stage1(k):
        x0(k).wait()
        r, s = k % R, k % RA
        for p in range(PARTS):
            v = bit(dim(p, k, 0))
            give = rows(p * PR + (1 - v) * (PR // 2), PR // 2)
            keep = rows(p * PR + v * (PR // 2), PR // 2)
            sb1[r, p] = (acc[s, pl.ds(give, PR // 2), :] + rb0[r, pl.ds(give, PR // 2), :].astype(F32)).astype(BF16)
            x1(k, p).start()
            acc[s, pl.ds(keep, PR // 2), :] += rb0[r, pl.ds(keep, PR // 2), :].astype(F32)

    def halve(k, i, x_in, x_out, rb, sb):
        r, s = k % R, k % RA
        m = PR // (2 * 2 ** i)
        for p in range(PARTS):
            x_in(k, p).wait()
            base = offs(k, p)[i - 1]
            v = bit(dim(p, k, i))
            give, keep = rows((1 - v) * m, m), rows(v * m, m)
            sb[r, p] = (acc[s, pl.ds(rows(base + give, m), m), :] + rb[r, p, pl.ds(give, m), :].astype(F32)).astype(BF16)
            x_out(k, p).start()
            acc[s, pl.ds(rows(base + keep, m), m), :] += rb[r, p, pl.ds(keep, m), :].astype(F32)

    def stage4(k):
        r, s = k % R, k % RA
        m = PR // 8
        for p in range(PARTS):
            x3(k, p).wait()
            o = rows(offs(k, p)[2], m)
            fb[r, p] = (acc[s, pl.ds(o, m), :] + rb3[r, p].astype(F32)).astype(BF16)
            y1(k, p).start()
            own(k, p).start()

    def stage5(k):
        for p in range(PARTS):
            own(k, p).wait()
            y1(k, p).wait()
            y2(k, p).start()

    def stage6(k):
        for p in range(PARTS):
            y2(k, p).wait()
            y3(k, p).start()

    def stage7(k):
        for p in range(PARTS):
            y3(k, p).wait()
        y4(k).start()

    def stage8(k):
        y4(k).wait()

    stages = (
        (D1, stage1),
        (D2, lambda k: halve(k, 1, x1, x2, rb1, sb2)),
        (D3, lambda k: halve(k, 2, x2, x3, rb2, sb3)),
        (D4, stage4), (D5, stage5), (D6, stage6), (D7, stage7), (D8, stage8))

    def half(u, _):
        k, h = u // 2, u % 2

        @pl.when(k < CH)
        def _():
            n, j = k // PER, k % PER
            hs = 2 * j + h

            @pl.when(h == 0)
            def _():
                g_copy(k).wait()

                @pl.when(k + 1 < CH)
                def _():
                    g_copy(k + 1).start()

            @pl.when(jnp.logical_and(hs == 0, n + 1 < N))
            def _():
                for q in range(2):
                    a_copy(n + 1, q, q).start()

            @pl.when(hs == 2 * (PER - 2))
            def _():
                rem_copy(n).start()

            slot = (1 - h) * RA + h * (k % RA)
            ro = rows((h * core + (1 - h) * (1 - core)) * H, H)
            acc[slot] = jnp.dot(aT[n % 2, pl.ds(ro, H), :], gv[k % 2], preferred_element_type=F32)

            @pl.when(jnp.logical_and(jnp.logical_and(hs >= 1, hs <= T // TB), n + 1 < N))
            def _():
                q = hs - 1
                a_copy(n + 1, q, q % 2).wait()
                transpose(n + 1, q, q % 2)

                @pl.when(q + 2 < T // TB)
                def _():
                    a_copy(n + 1, q + 2, q % 2).start()

            @pl.when(h == 0)
            def _():
                sb0[k % R] = acc[RA].astype(BF16)
                x0(k).start()

            @pl.when(j == PER - 1)
            def _():
                @pl.when(h == 0)
                def _():
                    rem_copy(n).wait()
                xacc[h, :, pl.ds(pl.multiple_of(n * REM, REM), REM)] = jnp.dot(
                    aT[n % 2, pl.ds(ro, H), :], grem[...], preferred_element_type=F32)

        @pl.when(u == 2 * CH)
        def _():
            sb0[k % R] = xacc[0].astype(BF16)
            x0(k).start()
            acc[k % RA] = xacc[1]

        for delay, stage in stages:
            w = u - delay

            @pl.when(jnp.logical_and(jnp.logical_and(w >= 0, w < 2 * NCH), (u + delay) % 2 == 0))
            def _():
                stage((u - delay) // 2)
        return 0

    lax.fori_loop(0, 2 * CH + D8 + 1, half, 0)


def place_kernel(c_ref, o_ref, buf, isem, osem):
    ins = [pltpu.make_async_copy(c_ref.at[k], buf.at[k], isem.at[k]) for k in range(NCH)]
    outs = []
    for k in range(CH):
        n, j = k // PER, k % PER
        outs.append([pltpu.make_async_copy(buf.at[k], o_ref.at[n, :, pl.ds(j * W, W)], osem.at[k])])
    outs.append([pltpu.make_async_copy(buf.at[CH, :, pl.ds(n * REM, REM)], o_ref.at[n, :, pl.ds(PER * W, REM)],
                                       osem.at[CH + n]) for n in range(N)])
    for c in ins:
        c.start()
    for c, o in zip(ins, outs):
        c.wait()
        for x in o:
            x.start()
    for o in outs:
        for x in o:
            x.wait()


def solution(mesh):
    def step(a, g):
        hbm = pl.BlockSpec(memory_space=pl.ANY)
        dma = pltpu.SemaphoreType.DMA
        chunks = pl.pallas_call(
            main_kernel,
            out_shape=jax.ShapeDtypeStruct((NCH, D, W), BF16),
            in_specs=[hbm] * 2,
            out_specs=hbm,
            scratch_shapes=[
                pltpu.VMEM((2, D, T), BF16),
                pltpu.VMEM((2, TB, D), BF16),
                pltpu.VMEM((2, T, W), BF16),
                pltpu.VMEM((T, REM), BF16),
                pltpu.VMEM((RA + 1, H, W), F32),
                pltpu.VMEM((2, H, W), F32),
                pltpu.VMEM((R, H, W), BF16),
                pltpu.VMEM((R, H, W), BF16),
                pltpu.VMEM((R, PARTS, PR // 2, W), BF16),
                pltpu.VMEM((R, PARTS, PR // 2, W), BF16),
                pltpu.VMEM((R, PARTS, PR // 4, W), BF16),
                pltpu.VMEM((R, PARTS, PR // 4, W), BF16),
                pltpu.VMEM((R, PARTS, PR // 8, W), BF16),
                pltpu.VMEM((R, PARTS, PR // 8, W), BF16),
                pltpu.VMEM((R, PARTS, PR // 8, W), BF16),
                dma((8, R, PARTS)),
                dma((8, R, PARTS)),
                dma((2,)),
                dma((2,)),
                dma,
                dma((R, PARTS)),
            ],
            compiler_params=pltpu.CompilerParams(
                collective_id=0, has_side_effects=True, vmem_limit_bytes=62 * 2**20),
            name="sum_chunks",
        )(a, g)
        return pl.pallas_call(
            place_kernel,
            out_shape=jax.ShapeDtypeStruct((N, D, F), BF16),
            in_specs=[hbm],
            out_specs=hbm,
            scratch_shapes=[pltpu.VMEM((NCH, D, W), BF16), dma((NCH,)), dma((CH + N,))],
            compiler_params=pltpu.CompilerParams(vmem_limit_bytes=40 * 2**20),
            name="place_chunks",
        )(chunks)

    return jax.shard_map(step, mesh=mesh, in_specs=(P(("rep", "dp")), P(("rep", "dp"))), out_specs=P("rep"),
                         check_vma=False)
```

```python
import functools

import jax
import jax.numpy as jnp
from jax import lax
from jax.experimental import pallas as pl
from jax.experimental.pallas import tpu as pltpu
from jax.sharding import PartitionSpec as P

LOGICAL = pl.DeviceIdType.LOGICAL
F32 = jnp.float32
BF16 = jnp.bfloat16

N, T, D, F = 4, 4096, 1024, 3200
H = D // 2
W = 512
PER = F // W
REM = F - PER * W
CH = N * PER
NCH = CH + 1
PART = ((0, 160), (160, 160), (320, 192))
TB = 512
R = 4
RA = 8
RY = 8
D1, D2, D3, D4, D5 = 1, 3, 4, 6, 8
A, B, D6 = 7, 16, 8
END = 2 * NCH
DONE = (A * (END - 1 - D6)) // B + 1
L7, L8 = 3, 4
LAST = END + NCH - DONE + L8

for _k in range(NCH):
    _u = -(-_k * B // A) + D6 if _k < DONE else END + _k - DONE
    assert _u >= 2 * _k + D5


def shift(x, s):
    return lax.shift_right_arithmetic(x, jnp.int32(s)) if isinstance(x, jax.Array) else x >> s


def low(x, m):
    return lax.bitwise_and(x, jnp.int32(m - 1)) if isinstance(x, jax.Array) else x % m


def third(k):
    return shift(k * 43, 7)


def sixth(k):
    return shift(k * 43, 8)


def main_kernel(a_ref, g_ref, out_ref, aT, ast, gv, grem, acc, xacc, sb0, rb0, sb1, rb1, sb2, rb2, sb3, rb3, fb,
                ssem, rsem, s3sem, r3sem, s4sem, r4sem, asem, gsem, remsem, lsem):
    me = lax.axis_index("dp")
    core = me % 2
    other = me + 1 - 2 * core
    strides = (8, 4, 2)
    bits = [(me // s) % 2 for s in strides]
    peers = [me + s * (1 - 2 * v) for s, v in zip(strides, bits)]

    barrier = pltpu.get_barrier_semaphore()
    for peer in [other] + peers:
        pl.semaphore_signal(barrier, inc=1, device_id=peer, device_id_type=LOGICAL)

    def at(q, v):
        return v[0] + q * (v[1] - v[0]) + shift(q * (q - 1), 1) * (v[2] - 2 * v[1] + v[0])

    def turn(k):
        q = k - 3 * third(k)
        return ([at(q, peers[e:] + peers[:e]) for e in range(3)], [at(q, bits[e:] + bits[:e]) for e in range(3)])

    def rows(x, m):
        return pl.multiple_of(x, m)

    def lanes(x):
        return pl.multiple_of(x, 128)

    def send(src, dst, send_sem, recv_sem, peer):
        return pltpu.make_async_remote_copy(
            src_ref=src, dst_ref=dst, send_sem=send_sem, recv_sem=recv_sem, device_id=peer, device_id_type=LOGICAL)

    def a_copy(n, q, slot):
        return pltpu.make_async_copy(a_ref.at[0, n, pl.ds(rows(q * TB, TB), TB), :], ast.at[slot], asem.at[slot])

    def g_copy(k):
        n = sixth(k)
        j = k - PER * n
        s = low(k, 2)
        return pltpu.make_async_copy(g_ref.at[0, n, :, pl.ds(lanes(j * W), W)], gv.at[s], gsem.at[s])

    def rem_copy(n):
        return pltpu.make_async_copy(g_ref.at[0, n, :, pl.ds(PER * W, REM)], grem, remsem)

    def transpose(n, q, slot):
        aT[low(n, 2), :, pl.ds(rows(q * TB, TB), TB)] = ast[slot].T

    for q in range(2):
        a_copy(0, q, q).start()
    g_copy(0).start()

    def first(q, _):
        a_copy(0, q, low(q, 2)).wait()
        transpose(0, q, low(q, 2))

        @pl.when(q + 2 < T // TB)
        def _():
            a_copy(0, q + 2, low(q, 2)).start()
        return 0

    lax.fori_loop(0, T // TB, first, 0)
    pl.semaphore_wait(barrier, 4)

    def x0(k):
        r = low(k, R)
        return send(sb0.at[r], rb0.at[r], ssem.at[0, r], rsem.at[0, r], other)

    def y4(k):
        b = out_ref.at[k, pl.ds(rows(core * H, H), H), :]
        y = low(k, RY)
        return send(b, b, s4sem.at[y], r4sem.at[y], other)

    def wait_parts(ref, ssem, rsem):
        c = send(ref, ref, ssem, rsem, other)
        c.wait_send()
        c.wait_recv()

    def place(k, o, m, c, w):
        return out_ref.at[k, pl.ds(rows(core * H + o, 16), m), pl.ds(lanes(c), w)]

    def stage1(k):
        x0(k).wait()
        r, s = low(k, R), low(k, RA)
        peer, bit = turn(k)
        for p, (o, m) in enumerate(PART):
            v = bit[p]
            part = pl.ds(o, m)
            give, keep = (pl.ds(lanes(c * (W // 2)), W // 2) for c in (1 - v, v))
            sb1[r, part, :] = (acc[s, part, give] + rb0[r, part, give].astype(F32)).astype(BF16)
            send(sb1.at[r, part], rb1.at[r, part], ssem.at[1, r], rsem.at[1, r], peer[p]).start()
            acc[s, part, keep] += rb0[r, part, keep].astype(F32)

    def stage2(k):
        r, s = low(k, R), low(k, RA)
        peer, bit = turn(k)
        wait_parts(sb1.at[r], ssem.at[1, r], rsem.at[1, r])
        for p, (o, m) in enumerate(PART):
            c1, v = bit[p] * (W // 2), bit[(p + 1) % 3]
            part = pl.ds(o, m)
            give, keep = (pl.ds(lanes(c * (W // 4)), W // 4) for c in (1 - v, v))
            agive, akeep = (pl.ds(lanes(c1 + c * (W // 4)), W // 4) for c in (1 - v, v))
            sb2[r, part, :] = (acc[s, part, agive] + rb1[r, part, give].astype(F32)).astype(BF16)
            send(sb2.at[r, part], rb2.at[r, part], ssem.at[2, r], rsem.at[2, r], peer[(p + 1) % 3]).start()
            acc[s, part, akeep] += rb1[r, part, keep].astype(F32)

    def stage3(k):
        r, s = low(k, R), low(k, RA)
        peer, bit = turn(k)
        wait_parts(sb2.at[r], ssem.at[2, r], rsem.at[2, r])
        for p, (o, m) in enumerate(PART):
            part = pl.ds(o, m)
            cols = pl.ds(lanes(bit[p] * (W // 2) + bit[(p + 1) % 3] * (W // 4)), W // 4)
            sb3[r, part, :] = (acc[s, part, cols] + rb2[r, part, :].astype(F32)).astype(BF16)
            send(sb3.at[r, part], rb3.at[r, part], ssem.at[3, r], rsem.at[3, r], peer[(p + 2) % 3]).start()

    def stage4(k):
        r = low(k, R)
        peer, bit = turn(k)
        wait_parts(sb3.at[r], ssem.at[3, r], rsem.at[3, r])
        for p, (o, m) in enumerate(PART):
            part = pl.ds(o, m)
            fb[r, part, :] = (sb3[r, part, :].astype(F32) + rb3[r, part, :].astype(F32)).astype(BF16)
            b = place(k, o, m, bit[p] * (W // 2) + bit[(p + 1) % 3] * (W // 4), W // 4)
            send(fb.at[r, part], b, ssem.at[4, r], rsem.at[4, r], peer[(p + 1) % 3]).start()
            pltpu.make_async_copy(fb.at[r, part], b, lsem.at[r]).start()

    def stage5(k):
        r = low(k, R)
        pltpu.make_async_copy(fb.at[r], fb.at[r], lsem.at[r]).wait()
        wait_parts(sb3.at[r], ssem.at[4, r], rsem.at[4, r])

    def stage6(k):
        y = low(k, RY)
        peer, bit = turn(k)
        for p, (o, m) in enumerate(PART):
            b = place(k, o, m, bit[p] * (W // 2), W // 2)
            send(b, b, s3sem.at[y], r3sem.at[y], peer[p]).start()

    def stage7(k):
        y = low(k, RY)
        wait_parts(sb1.at[0], s3sem.at[y], r3sem.at[y])
        y4(k).start()

    def stage8(k):
        y4(k).wait()

    stages = ((D2, stage2), (D3, stage3), (D4, stage4), (D1, stage1), (D5, stage5))
    slower = ((0, stage6), (L7, stage7), (L8, stage8))

    def half(u, _):
        k, h = shift(u, 1), low(u, 2)

        @pl.when(k < CH)
        def _():
            n = sixth(k)
            j = k - PER * n
            hs = 2 * j + h
            gs, ns = low(k, 2), low(n, 2)

            @pl.when(h == 0)
            def _():
                g_copy(k).wait()

                @pl.when(k + 1 < CH)
                def _():
                    g_copy(k + 1).start()

            @pl.when(jnp.logical_and(hs == 0, n + 1 < N))
            def _():
                for q in range(2):
                    a_copy(n + 1, q, q).start()

            @pl.when(hs == 2 * (PER - 2))
            def _():
                rem_copy(n).start()

            slot = (1 - h) * RA + h * low(k, RA)
            ro = rows((h * core + (1 - h) * (1 - core)) * H, H)
            acc[slot] = jnp.dot(aT[ns, pl.ds(ro, H), :], gv[gs], preferred_element_type=F32)

            @pl.when(jnp.logical_and(jnp.logical_and(hs >= 1, hs <= T // TB), n + 1 < N))
            def _():
                q = hs - 1
                qs = low(q, 2)
                a_copy(n + 1, q, qs).wait()
                transpose(n + 1, q, qs)

                @pl.when(q + 2 < T // TB)
                def _():
                    a_copy(n + 1, q + 2, qs).start()

            @pl.when(h == 0)
            def _():
                sb0[low(k, R)] = acc[RA].astype(BF16)
                x0(k).start()

            @pl.when(j == PER - 1)
            def _():
                @pl.when(h == 0)
                def _():
                    rem_copy(n).wait()
                xacc[h, :, pl.ds(lanes(n * REM), REM)] = jnp.dot(
                    aT[ns, pl.ds(ro, H), :], grem[...], preferred_element_type=F32)

        @pl.when(u == 2 * CH)
        def _():
            sb0[low(k, R)] = xacc[0].astype(BF16)
            x0(k).start()
            acc[low(k, RA)] = xacc[1]

        for delay, stage in stages:
            w = u - delay

            @pl.when(jnp.logical_and(jnp.logical_and(w >= 0, w < 2 * NCH), low(w, 2) == 0))
            def _():
                stage(shift(w, 1))
        for lag, stage in slower:
            v = u - lag
            w = A * (v - D6)
            early = jnp.logical_and(v < END, jnp.logical_and(w >= 0, low(w, B) < A))
            late = jnp.logical_and(v >= END, v < END + NCH - DONE)

            @pl.when(jnp.logical_or(early, late))
            def _():
                over = jnp.maximum(v - END + 1, 0)
                stage(jnp.where(over > 0, DONE - 1 + over, shift(w, 4)))
        return 0

    lax.fori_loop(0, LAST, half, 0)


def place_kernel(c_ref, o_ref, buf, isem, osem):
    ins = [pltpu.make_async_copy(c_ref.at[k], buf.at[k], isem.at[k]) for k in range(NCH)]
    outs = []
    for k in range(CH):
        n, j = k // PER, k % PER
        outs.append([pltpu.make_async_copy(buf.at[k], o_ref.at[n, :, pl.ds(j * W, W)], osem.at[k])])
    outs.append([pltpu.make_async_copy(buf.at[CH, :, pl.ds(n * REM, REM)], o_ref.at[n, :, pl.ds(PER * W, REM)],
                                       osem.at[CH + n]) for n in range(N)])
    for c in ins:
        c.start()
    for c, o in zip(ins, outs):
        c.wait()
        for x in o:
            x.start()
    for o in outs:
        for x in o:
            x.wait()


def solution(mesh):
    def step(a, g):
        hbm = pl.BlockSpec(memory_space=pl.ANY)
        dma = pltpu.SemaphoreType.DMA
        chunks = pl.pallas_call(
            main_kernel,
            out_shape=jax.ShapeDtypeStruct((NCH, D, W), BF16),
            in_specs=[hbm] * 2,
            out_specs=hbm,
            scratch_shapes=[
                pltpu.VMEM((2, D, T), BF16),
                pltpu.VMEM((2, TB, D), BF16),
                pltpu.VMEM((2, T, W), BF16),
                pltpu.VMEM((T, REM), BF16),
                pltpu.VMEM((RA + 1, H, W), F32),
                pltpu.VMEM((2, H, W), F32),
                pltpu.VMEM((R, H, W), BF16),
                pltpu.VMEM((R, H, W), BF16),
                pltpu.VMEM((R, H, W // 2), BF16),
                pltpu.VMEM((R, H, W // 2), BF16),
                pltpu.VMEM((R, H, W // 4), BF16),
                pltpu.VMEM((R, H, W // 4), BF16),
                pltpu.VMEM((R, H, W // 4), BF16),
                pltpu.VMEM((R, H, W // 4), BF16),
                pltpu.VMEM((R, H, W // 4), BF16),
                dma((5, R)),
                dma((5, R)),
                dma((RY,)),
                dma((RY,)),
                dma((RY,)),
                dma((RY,)),
                dma((2,)),
                dma((2,)),
                dma,
                dma((R,)),
            ],
            compiler_params=pltpu.CompilerParams(
                collective_id=0, has_side_effects=True, vmem_limit_bytes=62 * 2**20),
            name="sum_chunks",
        )(a, g)
        return pl.pallas_call(
            place_kernel,
            out_shape=jax.ShapeDtypeStruct((N, D, F), BF16),
            in_specs=[hbm],
            out_specs=hbm,
            scratch_shapes=[pltpu.VMEM((NCH, D, W), BF16), dma((NCH,)), dma((CH + N,))],
            compiler_params=pltpu.CompilerParams(vmem_limit_bytes=40 * 2**20),
            name="place_chunks",
        )(chunks)

    return jax.shard_map(step, mesh=mesh, in_specs=(P(("rep", "dp")), P(("rep", "dp"))), out_specs=P("rep"),
                         check_vma=False)
```

```python
import functools

import jax
import jax.numpy as jnp
from jax import lax
from jax.experimental import pallas as pl
from jax.experimental.pallas import tpu as pltpu
from jax.sharding import PartitionSpec as P

LOGICAL = pl.DeviceIdType.LOGICAL
F32 = jnp.float32
BF16 = jnp.bfloat16

N, T, D, F = 4, 4096, 1024, 3200
H = D // 2
W = 512
PER = F // W
REM = F - PER * W
CH = N * PER
NCH = CH + 1
PART = ((0, 160), (160, 160), (320, 192))
TB = 512
R = 4
RA = 8
RY = 8
D1, D2, D3, D4, D5 = 1, 3, 6, 8, 10
A, B, D6 = 8, 16, 10
END = 2 * NCH + 10
DONE = (A * (END - 1 - D6)) // B + 1
L7, L8 = 4, 5
LAST = END + NCH - DONE + L8

for _k in range(NCH):
    _u = -(-_k * B // A) + D6 if _k < DONE else END + _k - DONE
    assert _u >= 2 * _k + D5


def shift(x, s):
    return lax.shift_right_arithmetic(x, jnp.int32(s)) if isinstance(x, jax.Array) else x >> s


def low(x, m):
    return lax.bitwise_and(x, jnp.int32(m - 1)) if isinstance(x, jax.Array) else x % m


def third(k):
    return shift(k * 43, 7)


def sixth(k):
    return shift(k * 43, 8)


def main_kernel(a_ref, g_ref, out_ref, aT, ast, gv, grem, acc, xacc, sb0, rb0, sb1, rb1, sb2, rb2, sb3, rb3, fb,
                ssem, rsem, s3sem, r3sem, s4sem, r4sem, asem, gsem, remsem, lsem):
    me = lax.axis_index("dp")
    core = me % 2
    other = me + 1 - 2 * core
    strides = (8, 4, 2)
    bits = [(me // s) % 2 for s in strides]
    peers = [me + s * (1 - 2 * v) for s, v in zip(strides, bits)]

    barrier = pltpu.get_barrier_semaphore()
    for peer in [other] + peers:
        pl.semaphore_signal(barrier, inc=1, device_id=peer, device_id_type=LOGICAL)

    def at(q, v):
        return v[0] + q * (v[1] - v[0]) + shift(q * (q - 1), 1) * (v[2] - 2 * v[1] + v[0])

    def turn(k):
        q = k - 3 * third(k)
        return ([at(q, peers[e:] + peers[:e]) for e in range(3)], [at(q, bits[e:] + bits[:e]) for e in range(3)])

    def rows(x, m):
        return pl.multiple_of(x, m)

    def lanes(x):
        return pl.multiple_of(x, 128)

    def send(src, dst, send_sem, recv_sem, peer):
        return pltpu.make_async_remote_copy(
            src_ref=src, dst_ref=dst, send_sem=send_sem, recv_sem=recv_sem, device_id=peer, device_id_type=LOGICAL)

    def a_copy(n, q, slot):
        return pltpu.make_async_copy(a_ref.at[0, n, pl.ds(rows(q * TB, TB), TB), :], ast.at[slot], asem.at[slot])

    def g_copy(k):
        n = sixth(k)
        j = k - PER * n
        s = low(k, 2)
        return pltpu.make_async_copy(g_ref.at[0, n, :, pl.ds(lanes(j * W), W)], gv.at[s], gsem.at[s])

    def rem_copy(n):
        return pltpu.make_async_copy(g_ref.at[0, n, :, pl.ds(PER * W, REM)], grem, remsem)

    def transpose(n, q, slot):
        aT[low(n, 2), :, pl.ds(rows(q * TB, TB), TB)] = ast[slot].T

    for q in range(4):
        a_copy(0, q, q).start()
    g_copy(0).start()

    def first(q, _):
        a_copy(0, q, low(q, 4)).wait()
        transpose(0, q, low(q, 4))

        @pl.when(q + 4 < T // TB)
        def _():
            a_copy(0, q + 4, low(q, 4)).start()
        return 0

    lax.fori_loop(0, T // TB, first, 0)
    pl.semaphore_wait(barrier, 4)

    def x0(k):
        r = low(k, R)
        return send(sb0.at[r], rb0.at[r], ssem.at[0, r], rsem.at[0, r], other)

    def y4(k):
        b = out_ref.at[k, pl.ds(rows(core * H, H), H), :]
        y = low(k, RY)
        return send(b, b, s4sem.at[y], r4sem.at[y], other)

    def wait_parts(ref, ssem, rsem):
        c = send(ref, ref, ssem, rsem, other)
        c.wait_send()
        c.wait_recv()

    def place(k, o, m, c, w):
        return out_ref.at[k, pl.ds(rows(core * H + o, 16), m), pl.ds(lanes(c), w)]

    def stage1(k):
        x0(k).wait()
        r, s = low(k, R), low(k, RA)
        peer, bit = turn(k)
        for p, (o, m) in enumerate(PART):
            v = bit[p]
            part = pl.ds(o, m)
            give, keep = (pl.ds(lanes(c * (W // 2)), W // 2) for c in (1 - v, v))
            sb1[r, part, :] = (acc[s, part, give] + rb0[r, part, give].astype(F32)).astype(BF16)
            send(sb1.at[r, part], rb1.at[r, part], ssem.at[1, r], rsem.at[1, r], peer[p]).start()
            acc[s, part, keep] += rb0[r, part, keep].astype(F32)

    def stage2(k):
        r, s = low(k, R), low(k, RA)
        peer, bit = turn(k)
        wait_parts(sb1.at[r], ssem.at[1, r], rsem.at[1, r])
        for p, (o, m) in enumerate(PART):
            c1, v = bit[p] * (W // 2), bit[(p + 1) % 3]
            part = pl.ds(o, m)
            give, keep = (pl.ds(lanes(c * (W // 4)), W // 4) for c in (1 - v, v))
            agive, akeep = (pl.ds(lanes(c1 + c * (W // 4)), W // 4) for c in (1 - v, v))
            sb2[r, part, :] = (acc[s, part, agive] + rb1[r, part, give].astype(F32)).astype(BF16)
            send(sb2.at[r, part], rb2.at[r, part], ssem.at[2, r], rsem.at[2, r], peer[(p + 1) % 3]).start()
            acc[s, part, akeep] += rb1[r, part, keep].astype(F32)

    def stage3(k):
        r, s = low(k, R), low(k, RA)
        peer, bit = turn(k)
        wait_parts(sb2.at[r], ssem.at[2, r], rsem.at[2, r])
        for p, (o, m) in enumerate(PART):
            part = pl.ds(o, m)
            cols = pl.ds(lanes(bit[p] * (W // 2) + bit[(p + 1) % 3] * (W // 4)), W // 4)
            sb3[r, part, :] = (acc[s, part, cols] + rb2[r, part, :].astype(F32)).astype(BF16)
            send(sb3.at[r, part], rb3.at[r, part], ssem.at[3, r], rsem.at[3, r], peer[(p + 2) % 3]).start()

    def stage4(k):
        r = low(k, R)
        peer, bit = turn(k)
        wait_parts(sb3.at[r], ssem.at[3, r], rsem.at[3, r])
        for p, (o, m) in enumerate(PART):
            part = pl.ds(o, m)
            fb[r, part, :] = (sb3[r, part, :].astype(F32) + rb3[r, part, :].astype(F32)).astype(BF16)
            b = place(k, o, m, bit[p] * (W // 2) + bit[(p + 1) % 3] * (W // 4), W // 4)
            send(fb.at[r, part], b, ssem.at[4, r], rsem.at[4, r], peer[(p + 1) % 3]).start()
            pltpu.make_async_copy(fb.at[r, part], b, lsem.at[r]).start()

    def stage5(k):
        r = low(k, R)
        pltpu.make_async_copy(fb.at[r], fb.at[r], lsem.at[r]).wait()
        wait_parts(sb3.at[r], ssem.at[4, r], rsem.at[4, r])

    def stage6(k):
        y = low(k, RY)
        peer, bit = turn(k)
        for p, (o, m) in enumerate(PART):
            b = place(k, o, m, bit[p] * (W // 2), W // 2)
            send(b, b, s3sem.at[y], r3sem.at[y], peer[p]).start()

    def stage7(k):
        y = low(k, RY)
        wait_parts(sb1.at[0], s3sem.at[y], r3sem.at[y])
        y4(k).start()

    def stage8(k):
        y4(k).wait()

    stages = ((D2, stage2), (D3, stage3), (D4, stage4), (D1, stage1), (D5, stage5))
    slower = ((0, stage6), (L7, stage7), (L8, stage8))

    def half(u, _):
        k, h = shift(u, 1), low(u, 2)

        @pl.when(k < CH)
        def _():
            n = sixth(k)
            j = k - PER * n
            hs = 2 * j + h
            gs, ns = low(k, 2), low(n, 2)

            @pl.when(h == 0)
            def _():
                g_copy(k).wait()

                @pl.when(k + 1 < CH)
                def _():
                    g_copy(k + 1).start()

            @pl.when(jnp.logical_and(hs == 0, n + 1 < N))
            def _():
                for q in range(2):
                    a_copy(n + 1, q, q).start()

            @pl.when(hs == 2 * (PER - 2))
            def _():
                rem_copy(n).start()

            slot = (1 - h) * RA + h * low(k, RA)
            ro = rows((h * core + (1 - h) * (1 - core)) * H, H)
            acc[slot] = jnp.dot(aT[ns, pl.ds(ro, H), :], gv[gs], preferred_element_type=F32)

            @pl.when(jnp.logical_and(jnp.logical_and(hs >= 1, hs <= T // TB), n + 1 < N))
            def _():
                q = hs - 1
                qs = low(q, 2)
                a_copy(n + 1, q, qs).wait()
                transpose(n + 1, q, qs)

                @pl.when(q + 2 < T // TB)
                def _():
                    a_copy(n + 1, q + 2, qs).start()

            @pl.when(h == 0)
            def _():
                sb0[low(k, R)] = acc[RA].astype(BF16)
                x0(k).start()

            @pl.when(j == PER - 1)
            def _():
                @pl.when(h == 0)
                def _():
                    rem_copy(n).wait()
                xacc[h, :, pl.ds(lanes(n * REM), REM)] = jnp.dot(
                    aT[ns, pl.ds(ro, H), :], grem[...], preferred_element_type=F32)

        @pl.when(u == 2 * CH)
        def _():
            sb0[low(k, R)] = xacc[0].astype(BF16)
            x0(k).start()
            acc[low(k, RA)] = xacc[1]

        for delay, stage in stages:
            w = u - delay

            @pl.when(jnp.logical_and(jnp.logical_and(w >= 0, w < 2 * NCH), low(w, 2) == 0))
            def _():
                stage(shift(w, 1))
        for lag, stage in slower:
            v = u - lag
            w = A * (v - D6)
            early = jnp.logical_and(v < END, jnp.logical_and(w >= 0, low(w, B) < A))
            late = jnp.logical_and(v >= END, v < END + NCH - DONE)

            @pl.when(jnp.logical_or(early, late))
            def _():
                over = jnp.maximum(v - END + 1, 0)
                stage(jnp.where(over > 0, DONE - 1 + over, shift(w, 4)))
        return 0

    lax.fori_loop(0, LAST, half, 0)


def place_kernel(c_ref, o_ref, buf, isem, osem):
    ins = [pltpu.make_async_copy(c_ref.at[k], buf.at[k], isem.at[k]) for k in range(NCH)]
    outs = []
    for k in range(CH):
        n, j = k // PER, k % PER
        outs.append([pltpu.make_async_copy(buf.at[k], o_ref.at[n, :, pl.ds(j * W, W)], osem.at[k])])
    outs.append([pltpu.make_async_copy(buf.at[CH, :, pl.ds(n * REM, REM)], o_ref.at[n, :, pl.ds(PER * W, REM)],
                                       osem.at[CH + n]) for n in range(N)])
    for c in ins:
        c.start()
    for c, o in zip(ins, outs):
        c.wait()
        for x in o:
            x.start()
    for o in outs:
        for x in o:
            x.wait()


def solution(mesh):
    def step(a, g):
        hbm = pl.BlockSpec(memory_space=pl.ANY)
        dma = pltpu.SemaphoreType.DMA
        chunks = pl.pallas_call(
            main_kernel,
            out_shape=jax.ShapeDtypeStruct((NCH, D, W), BF16),
            in_specs=[hbm] * 2,
            out_specs=hbm,
            scratch_shapes=[
                pltpu.VMEM((2, D, T), BF16),
                pltpu.VMEM((4, TB, D), BF16),
                pltpu.VMEM((2, T, W), BF16),
                pltpu.VMEM((T, REM), BF16),
                pltpu.VMEM((RA + 1, H, W), F32),
                pltpu.VMEM((2, H, W), F32),
                pltpu.VMEM((R, H, W), BF16),
                pltpu.VMEM((R, H, W), BF16),
                pltpu.VMEM((R, H, W // 2), BF16),
                pltpu.VMEM((R, H, W // 2), BF16),
                pltpu.VMEM((R, H, W // 4), BF16),
                pltpu.VMEM((R, H, W // 4), BF16),
                pltpu.VMEM((R, H, W // 4), BF16),
                pltpu.VMEM((R, H, W // 4), BF16),
                pltpu.VMEM((R, H, W // 4), BF16),
                dma((5, R)),
                dma((5, R)),
                dma((RY,)),
                dma((RY,)),
                dma((RY,)),
                dma((RY,)),
                dma((4,)),
                dma((2,)),
                dma,
                dma((R,)),
            ],
            compiler_params=pltpu.CompilerParams(
                collective_id=0, has_side_effects=True, vmem_limit_bytes=62 * 2**20),
            name="sum_chunks",
        )(a, g)
        return pl.pallas_call(
            place_kernel,
            out_shape=jax.ShapeDtypeStruct((N, D, F), BF16),
            in_specs=[hbm],
            out_specs=hbm,
            scratch_shapes=[pltpu.VMEM((NCH, D, W), BF16), dma((NCH,)), dma((CH + N,))],
            compiler_params=pltpu.CompilerParams(vmem_limit_bytes=40 * 2**20),
            name="place_chunks",
        )(chunks)

    return jax.shard_map(step, mesh=mesh, in_specs=(P(("rep", "dp")), P(("rep", "dp"))), out_specs=P("rep"),
                         check_vma=False)
```

```python
import functools

import jax
import jax.numpy as jnp
from jax import lax
from jax.experimental import pallas as pl
from jax.experimental.pallas import tpu as pltpu
from jax.sharding import PartitionSpec as P

LOGICAL = pl.DeviceIdType.LOGICAL
F32 = jnp.float32
BF16 = jnp.bfloat16

N, T, D, F = 4, 4096, 1024, 3200
H = D // 2
W = 512
PER = F // W
REM = F - PER * W
CH = N * PER
NCH = CH + 1
PART = ((0, 160), (160, 160), (320, 192))
TB = 512
R = 4
RA = 8
RY = 8
D1, D2, D3, D4, D5 = 1, 3, 6, 8, 10
A, B, D6 = 8, 16, 10
END = 2 * NCH + 10
DONE = (A * (END - 1 - D6)) // B + 1
L7, L8 = 4, 5
LAST = END + NCH - DONE + L8

for _k in range(NCH):
    _u = -(-_k * B // A) + D6 if _k < DONE else END + _k - DONE
    assert _u >= 2 * _k + D5


def shift(x, s):
    return lax.shift_right_arithmetic(x, jnp.int32(s)) if isinstance(x, jax.Array) else x >> s


def low(x, m):
    return lax.bitwise_and(x, jnp.int32(m - 1)) if isinstance(x, jax.Array) else x % m


def third(k):
    return shift(k * 43, 7)


def sixth(k):
    return shift(k * 43, 8)


def main_kernel(a_ref, g_ref, out_ref, aT, ast, gv, grem, acc, xacc, sb0, rb0, sb1, rb1, sb2, rb2, sb3, rb3, fb,
                ssem, rsem, s3sem, r3sem, s4sem, r4sem, asem, gsem, remsem, lsem):
    me = lax.axis_index("dp")
    core = me % 2
    other = me + 1 - 2 * core
    strides = (8, 4, 2)
    bits = [(me // s) % 2 for s in strides]
    peers = [me + s * (1 - 2 * v) for s, v in zip(strides, bits)]

    barrier = pltpu.get_barrier_semaphore()
    for peer in [other] + peers:
        pl.semaphore_signal(barrier, inc=1, device_id=peer, device_id_type=LOGICAL)

    def at(q, v):
        return v[0] + q * (v[1] - v[0]) + shift(q * (q - 1), 1) * (v[2] - 2 * v[1] + v[0])

    def turn(k):
        q = k - 3 * third(k)
        return ([at(q, peers[e:] + peers[:e]) for e in range(3)], [at(q, bits[e:] + bits[:e]) for e in range(3)])

    def rows(x, m):
        return pl.multiple_of(x, m)

    def lanes(x):
        return pl.multiple_of(x, 128)

    def send(src, dst, send_sem, recv_sem, peer):
        return pltpu.make_async_remote_copy(
            src_ref=src, dst_ref=dst, send_sem=send_sem, recv_sem=recv_sem, device_id=peer, device_id_type=LOGICAL)

    def a_copy(n, q, slot):
        return pltpu.make_async_copy(a_ref.at[0, n, pl.ds(rows(q * TB, TB), TB), :], ast.at[slot], asem.at[slot])

    def g_copy(k):
        n = sixth(k)
        j = k - PER * n
        s = low(k, 2)
        return pltpu.make_async_copy(g_ref.at[0, n, :, pl.ds(lanes(j * W), W)], gv.at[s], gsem.at[s])

    def rem_copy(n):
        return pltpu.make_async_copy(g_ref.at[0, n, :, pl.ds(PER * W, REM)], grem, remsem)

    def transpose(n, q, slot):
        aT[low(n, 2), :, pl.ds(rows(q * TB, TB), TB)] = ast[slot].T

    for q in range(4):
        a_copy(0, q, q).start()
    g_copy(0).start()

    def first(q, _):
        a_copy(0, q, low(q, 4)).wait()
        transpose(0, q, low(q, 4))

        @pl.when(q + 4 < T // TB)
        def _():
            a_copy(0, q + 4, low(q, 4)).start()
        return 0

    lax.fori_loop(0, T // TB, first, 0)
    pl.semaphore_wait(barrier, 4)

    def x0(k):
        r = low(k, R)
        return send(sb0.at[r], rb0.at[r], ssem.at[0, r], rsem.at[0, r], other)

    def y4(k):
        b = out_ref.at[k, pl.ds(rows(core * H, H), H), :]
        y = low(k, RY)
        return send(b, b, s4sem.at[y], r4sem.at[y], other)

    def wait_parts(ref, ssem, rsem):
        c = send(ref, ref, ssem, rsem, other)
        c.wait_send()
        c.wait_recv()

    def place(k, o, m, c, w):
        return out_ref.at[k, pl.ds(rows(core * H + o, 16), m), pl.ds(lanes(c), w)]

    def stage1(k):
        x0(k).wait()
        r, s = low(k, R), low(k, RA)
        peer, bit = turn(k)
        for p, (o, m) in enumerate(PART):
            v = bit[p]
            part = pl.ds(o, m)
            give, keep = (pl.ds(lanes(c * (W // 2)), W // 2) for c in (1 - v, v))
            sb1[r, part, :] = (acc[s, part, give] + rb0[r, part, give].astype(F32)).astype(BF16)
            send(sb1.at[r, part], rb1.at[r, part], ssem.at[1, r], rsem.at[1, r], peer[p]).start()
            acc[s, part, keep] += rb0[r, part, keep].astype(F32)

    def stage2(k):
        r, s = low(k, R), low(k, RA)
        peer, bit = turn(k)
        wait_parts(sb1.at[r], ssem.at[1, r], rsem.at[1, r])
        for p, (o, m) in enumerate(PART):
            c1, v = bit[p] * (W // 2), bit[(p + 1) % 3]
            part = pl.ds(o, m)
            give, keep = (pl.ds(lanes(c * (W // 4)), W // 4) for c in (1 - v, v))
            agive, akeep = (pl.ds(lanes(c1 + c * (W // 4)), W // 4) for c in (1 - v, v))
            sb2[r, part, :] = (acc[s, part, agive] + rb1[r, part, give].astype(F32)).astype(BF16)
            send(sb2.at[r, part], rb2.at[r, part], ssem.at[2, r], rsem.at[2, r], peer[(p + 1) % 3]).start()
            acc[s, part, akeep] += rb1[r, part, keep].astype(F32)

    def stage3(k):
        r, s = low(k, R), low(k, RA)
        peer, bit = turn(k)
        wait_parts(sb2.at[r], ssem.at[2, r], rsem.at[2, r])
        for p, (o, m) in enumerate(PART):
            part = pl.ds(o, m)
            cols = pl.ds(lanes(bit[p] * (W // 2) + bit[(p + 1) % 3] * (W // 4)), W // 4)
            sb3[r, part, :] = (acc[s, part, cols] + rb2[r, part, :].astype(F32)).astype(BF16)
            send(sb3.at[r, part], rb3.at[r, part], ssem.at[3, r], rsem.at[3, r], peer[(p + 2) % 3]).start()

    def stage4(k):
        r = low(k, R)
        peer, bit = turn(k)
        wait_parts(sb3.at[r], ssem.at[3, r], rsem.at[3, r])
        for p, (o, m) in enumerate(PART):
            part = pl.ds(o, m)
            fb[r, part, :] = (sb3[r, part, :].astype(F32) + rb3[r, part, :].astype(F32)).astype(BF16)
            b = place(k, o, m, bit[p] * (W // 2) + bit[(p + 1) % 3] * (W // 4), W // 4)
            send(fb.at[r, part], b, ssem.at[4, r], rsem.at[4, r], peer[(p + 1) % 3]).start()
            pltpu.make_async_copy(fb.at[r, part], b, lsem.at[r]).start()

    def stage5(k):
        r = low(k, R)
        pltpu.make_async_copy(fb.at[r], fb.at[r], lsem.at[r]).wait()
        wait_parts(sb3.at[r], ssem.at[4, r], rsem.at[4, r])

    def stage6(k):
        y = low(k, RY)
        peer, bit = turn(k)
        for p, (o, m) in enumerate(PART):
            b = place(k, o, m, bit[p] * (W // 2), W // 2)
            send(b, b, s3sem.at[y], r3sem.at[y], peer[p]).start()

    def stage7(k):
        y = low(k, RY)
        wait_parts(sb1.at[0], s3sem.at[y], r3sem.at[y])
        y4(k).start()

    def stage8(k):
        y4(k).wait()

    stages = ((D2, stage2), (D3, stage3), (D4, stage4), (D1, stage1), (D5, stage5))
    slower = ((0, stage6), (L7, stage7), (L8, stage8))

    def half(u, _):
        k, h = shift(u, 1), low(u, 2)

        @pl.when(k < CH)
        def _():
            n = sixth(k)
            j = k - PER * n
            hs = 2 * j + h
            gs, ns = low(k, 2), low(n, 2)

            @pl.when(h == 0)
            def _():
                g_copy(k).wait()

                @pl.when(k + 1 < CH)
                def _():
                    g_copy(k + 1).start()

            @pl.when(jnp.logical_and(hs == 0, n + 1 < N))
            def _():
                for q in range(2):
                    a_copy(n + 1, q, q).start()

            @pl.when(hs == 2 * (PER - 2))
            def _():
                rem_copy(n).start()

            slot = (1 - h) * RA + h * low(k, RA)
            ro = rows((h * core + (1 - h) * (1 - core)) * H, H)
            acc[slot] = jnp.dot(aT[ns, pl.ds(ro, H), :], gv[gs], preferred_element_type=F32)

            @pl.when(jnp.logical_and(jnp.logical_and(hs >= 1, hs <= T // TB), n + 1 < N))
            def _():
                q = hs - 1
                qs = low(q, 2)
                a_copy(n + 1, q, qs).wait()
                transpose(n + 1, q, qs)

                @pl.when(q + 2 < T // TB)
                def _():
                    a_copy(n + 1, q + 2, qs).start()

            @pl.when(h == 0)
            def _():
                sb0[low(k, R)] = acc[RA].astype(BF16)
                x0(k).start()

            @pl.when(j == PER - 1)
            def _():
                @pl.when(h == 0)
                def _():
                    rem_copy(n).wait()
                xacc[h, :, pl.ds(lanes(n * REM), REM)] = jnp.dot(
                    aT[ns, pl.ds(ro, H), :], grem[...], preferred_element_type=F32)

        @pl.when(u == 2 * CH)
        def _():
            sb0[low(k, R)] = xacc[0].astype(BF16)
            x0(k).start()
            acc[low(k, RA)] = xacc[1]

        for delay, stage in stages:
            w = u - delay

            @pl.when(jnp.logical_and(jnp.logical_and(w >= 0, w < 2 * NCH), low(w, 2) == 0))
            def _():
                stage(shift(w, 1))
        for lag, stage in slower:
            v = u - lag
            w = A * (v - D6)
            early = jnp.logical_and(v < END, jnp.logical_and(w >= 0, low(w, B) < A))
            late = jnp.logical_and(v >= END, v < END + NCH - DONE)

            @pl.when(jnp.logical_or(early, late))
            def _():
                over = jnp.maximum(v - END + 1, 0)
                stage(jnp.where(over > 0, DONE - 1 + over, shift(w, 4)))
        return 0

    lax.fori_loop(0, LAST, half, 0)


def place_kernel(c_ref, o_ref, buf, isem, osem):
    ins = [pltpu.make_async_copy(c_ref.at[k], buf.at[k], isem.at[k]) for k in range(NCH)]
    outs = []
    for k in range(CH):
        n, j = k // PER, k % PER
        outs.append([pltpu.make_async_copy(buf.at[k], o_ref.at[n, :, pl.ds(j * W, W)], osem)])
    outs.append([pltpu.make_async_copy(buf.at[CH, :, pl.ds(n * REM, REM)], o_ref.at[n, :, pl.ds(PER * W, REM)],
                                       osem) for n in range(N)])
    for c in ins:
        c.start()
    for c, o in zip(ins, outs):
        c.wait()
        for x in o:
            x.start()
    pltpu.make_async_copy(o_ref, o_ref, osem).wait()


def solution(mesh):
    def step(a, g):
        hbm = pl.BlockSpec(memory_space=pl.ANY)
        dma = pltpu.SemaphoreType.DMA
        chunks = pl.pallas_call(
            main_kernel,
            out_shape=jax.ShapeDtypeStruct((NCH, D, W), BF16),
            in_specs=[hbm] * 2,
            out_specs=hbm,
            scratch_shapes=[
                pltpu.VMEM((2, D, T), BF16),
                pltpu.VMEM((4, TB, D), BF16),
                pltpu.VMEM((2, T, W), BF16),
                pltpu.VMEM((T, REM), BF16),
                pltpu.VMEM((RA + 1, H, W), F32),
                pltpu.VMEM((2, H, W), F32),
                pltpu.VMEM((R, H, W), BF16),
                pltpu.VMEM((R, H, W), BF16),
                pltpu.VMEM((R, H, W // 2), BF16),
                pltpu.VMEM((R, H, W // 2), BF16),
                pltpu.VMEM((R, H, W // 4), BF16),
                pltpu.VMEM((R, H, W // 4), BF16),
                pltpu.VMEM((R, H, W // 4), BF16),
                pltpu.VMEM((R, H, W // 4), BF16),
                pltpu.VMEM((R, H, W // 4), BF16),
                dma((5, R)),
                dma((5, R)),
                dma((RY,)),
                dma((RY,)),
                dma((RY,)),
                dma((RY,)),
                dma((4,)),
                dma((2,)),
                dma,
                dma((R,)),
            ],
            compiler_params=pltpu.CompilerParams(
                collective_id=0, has_side_effects=True, vmem_limit_bytes=62 * 2**20),
            name="sum_chunks",
        )(a, g)
        return pl.pallas_call(
            place_kernel,
            out_shape=jax.ShapeDtypeStruct((N, D, F), BF16),
            in_specs=[hbm],
            out_specs=hbm,
            scratch_shapes=[pltpu.VMEM((NCH, D, W), BF16), dma((NCH,)), dma],
            compiler_params=pltpu.CompilerParams(vmem_limit_bytes=40 * 2**20),
            name="place_chunks",
        )(chunks)

    return jax.shard_map(step, mesh=mesh, in_specs=(P(("rep", "dp")), P(("rep", "dp"))), out_specs=P("rep"),
                         check_vma=False)
```
